256 devices in a mesh: member: 8 (over y, x_lo), space: 32 (over z, x_hi, core).
Axes of the slice: x: 4 (x_hi: 2, x_lo: 2; x = x_hi * 2 + x_lo), y: 4, z: 8, core: 2. Of those that a mesh axis runs over, the one named last changes fastest.
Arguments:
- hidden_codes: bfloat16 [16, 256, 92160], P('member', None, 'space'), may hold values from -6 to 6
- w_in: bfloat16 [1024, 256], replicated, may hold values from -0.375 to 0.375
- b_in: float32 [1024], replicated, may hold values from -3 to 3
- w_out: bfloat16 [72, 1024], replicated, may hold values from -0.1875 to 0.1875
- b_out: float32 [72], replicated, may hold values from -3 to 3
- target: bfloat16 [72, 92160], P(None, 'space'), may hold values from -6 to 6
- band_start: int32 [32], P('space'), may hold values from 0 to 62, as said below
Outputs:
- code_sensitivity: bfloat16 [16, 256, 92160], P('member', None, 'space')
- grad_w_in: float32 [1024, 256], replicated
- grad_w_out: float32 [72, 1024], replicated
- grad_b_in: float32 [1024], replicated
The draws below stay inside these ranges and needn't reach their ends.
Inputs may be any that keep to these rules, and one draw needn't show every extreme that they name: band_start holds each of 0, 2, 4, ... once, in some order.
All inputs are finite; a program needn't handle non-finite values.
Results may differ from the reference program's by a relative error of at most 0.005.
The reference program's roundings to bfloat16 on the way count: a program that leaves them out, or rounds other values in their place, can miss the bound.
Values may be sent and summed in bfloat16 or wider, within the bound.
No kernel may reach another device: no remote copies, remote signals or barrier semaphores. Data moves between devices by JAX's collectives and lax.ppermute only.
A program may use at most 128 MiB of HBM per device.

```python
import math
import jax
import jax.numpy as jnp
from jax import lax

CHANNELS = 72
HID = 1024
LATENT = 256
LON = 1440
ROWS_DEV = 2
MEMBERS = 16
CELLS = 92160
N_SPACE = 32


def draw_band_start(key, part):
    order = jax.random.permutation(jax.random.fold_in(key, 11), N_SPACE)
    return (order * ROWS_DEV).astype(jnp.int32)


def level_of(rng, dims, cuts, smallest, high):
    def one(dim, parts):
        heights = jax.random.uniform(jax.random.fold_in(jax.random.fold_in(rng, 6), dim), (parts,), jnp.float32, smallest / len(cuts), high / len(cuts))
        return jnp.repeat(jnp.exp(heights), dims[dim] // parts).reshape((-1,) + (1,) * (len(dims) - dim - 1))

    level = one(*cuts[0])
    for cut in cuts[1:]:
        level = level * one(*cut)
    return level


def bell_draw(rng, dims, scale, reach, split=(), kind=jnp.bfloat16):
    factor_of = level_of(rng, dims, split, -0.22, 0.18) if split else 1.0
    values = jax.random.normal(rng, dims, jnp.float32) * scale * factor_of
    return jnp.minimum(jnp.maximum(values, -reach), reach).astype(kind)


def setup_inputs(seed: int = 0) -> dict:
    key_list = jax.random.split(jax.random.key(seed), 8)
    hidden_codes = bell_draw(key_list[0], (MEMBERS, LATENT, CELLS), 1.0, 6.0, ((0, 8), (2, 32)))
    w_in = bell_draw(key_list[1], (HID, LATENT), LATENT ** -0.5, 0.375)
    b_in = bell_draw(key_list[2], (HID,), 0.5, 3.0, (), jnp.float32)
    w_out = bell_draw(key_list[3], (CHANNELS, HID), HID ** -0.5, 0.1875)
    b_out = bell_draw(key_list[4], (CHANNELS,), 0.5, 3.0, (), jnp.float32)
    target = bell_draw(key_list[5], (CHANNELS, CELLS), 1.0, 6.0, ((1, 32),))
    band_start = draw_band_start(jax.random.fold_in(key_list[7], 71), 0)
    return dict(hidden_codes=hidden_codes, w_in=w_in, b_in=b_in, w_out=w_out, b_out=b_out, target=target, band_start=band_start)


def slope(diff):
    return diff / jnp.sqrt(diff * diff + 0.0625)

def area_weights(band_start):
    rows = band_start[:, None] + jnp.arange(ROWS_DEV, dtype=jnp.int32)[None, :]
    angle = (rows.astype(jnp.float32) + 0.5) * (math.pi / (ROWS_DEV * N_SPACE)) - math.pi / 2
    return jnp.repeat(jnp.cos(angle).reshape(-1), LON)

def reference(hidden_codes, w_in, b_in, w_out, b_out, target, band_start):
    area = area_weights(band_start)
    members = hidden_codes.shape[0]
    cells = hidden_codes.shape[2]

    def apply_readout(inputs):
        pre = jnp.dot(w_in, inputs, preferred_element_type=jnp.float32) + b_in[:, None]
        act = jax.nn.gelu(pre).astype(jnp.bfloat16)
        return (jnp.dot(w_out, act, preferred_element_type=jnp.float32) + b_out[:, None]).astype(jnp.bfloat16)
    predicted_maps = lax.map(apply_readout, hidden_codes)
    goal = target.astype(jnp.float32)

    def cross_sensitivity(mine):
        diagonal_contribution = mine.astype(jnp.float32)

        def lone_realization(total, other):
            return (total + slope(diagonal_contribution - other.astype(jnp.float32)), None)
        couple_index, discarded_value = lax.scan(lone_realization, jnp.zeros_like(diagonal_contribution), predicted_maps)
        return (area[None, :] * (slope(diagonal_contribution - goal) - couple_index / members)).astype(jnp.bfloat16)
    prediction_sensitivity = lax.map(cross_sensitivity, predicted_maps)

    def reverse_sweep(carry, items):
        inputs, prediction_adjoint = items
        pre = jnp.dot(w_in, inputs, preferred_element_type=jnp.float32) + b_in[:, None]
        act_f, undo = jax.vjp(jax.nn.gelu, pre)
        act = act_f.astype(jnp.bfloat16)
        dact = jnp.dot(w_out.T, prediction_adjoint, preferred_element_type=jnp.float32)
        dpre = undo(dact)[0].astype(jnp.bfloat16)
        dlat = jnp.dot(w_in.T, dpre, preferred_element_type=jnp.float32).astype(jnp.bfloat16)
        adjoint_entry_matrix = carry[0] + jnp.dot(dpre, inputs.T, preferred_element_type=jnp.float32)
        adjoint_exit_matrix = carry[1] + jnp.dot(prediction_adjoint, act.T, preferred_element_type=jnp.float32)
        adjoint_offset = carry[2] + lax.optimization_barrier(jnp.sum(dpre.astype(jnp.float32), axis=1))
        return ((adjoint_entry_matrix, adjoint_exit_matrix, adjoint_offset), dlat)
    opening_offset = (jnp.zeros(w_in.shape, jnp.float32), jnp.zeros(w_out.shape, jnp.float32), jnp.zeros(b_in.shape, jnp.float32))
    (adjoint_entry_matrix, adjoint_exit_matrix, adjoint_offset), code_sensitivity = lax.scan(reverse_sweep, opening_offset, (hidden_codes, prediction_sensitivity))
    scale = 1.0 / math.sqrt(members * (cells // N_SPACE))
    return (code_sensitivity, adjoint_entry_matrix * scale, adjoint_exit_matrix * scale, adjoint_offset * scale)
```

```python
import math

import jax
import jax.numpy as jnp
from jax import lax
from jax.experimental import pallas as pl
from jax.experimental.pallas import tpu as pltpu
from jax.sharding import Mesh
from jax.sharding import PartitionSpec as P

LON = 1440
BLK = 768
SUB = 256
C0 = math.sqrt(2.0 / math.pi)
C1 = C0 * 0.044715
F32 = jnp.float32
BF16 = jnp.bfloat16

FINE = (("y", 4), ("xl", 2), ("z", 8), ("xh", 2), ("c", 2))
MEMBER = ("y", "xl")
SPACE = ("z", "xh", "c")
CHIPS = ("y", "xl", "z", "xh")


def fwd_kernel(cells, hc_ref, w_in_ref, b_ref, w_out_ref, bo_ref, f_ref, act_ref, gp_ref):
    hid = w_in_ref.shape[0]
    hc = hc_ref[0]
    lane = lax.broadcasted_iota(jnp.int32, hc.shape, 1) + pl.program_id(1) * BLK
    hc = jnp.where(lane < cells, hc, jnp.zeros_like(hc))
    for k in range(hid // SUB):
        rows = pl.ds(k * SUB, SUB)
        pre = jnp.dot(w_in_ref[rows, :], hc, preferred_element_type=F32)
        x = pre + jnp.concatenate([b_ref[rows, :]] * (BLK // 128), axis=1)
        x2 = x * x
        t = jnp.tanh(x * (C1 * x2 + C0))
        h = 0.5 * t + 0.5
        a = x * h
        g = a * (1.0 - h) * ((6.0 * C1) * x2 + 2.0 * C0) + h
        act_ref[0, rows, :] = a.astype(BF16)
        gp_ref[0, rows, :] = g.astype(BF16)
    f = jnp.dot(w_out_ref[...], act_ref[0], preferred_element_type=F32)
    f = (f + bo_ref[...]).astype(BF16)
    half = BLK // 2
    f_ref[0, 0] = f[:, :half]
    f_ref[1, 0] = f[:, half:]


def decoder_forward(hidden_codes, w_in, b_wide, w_out, b_out):
    members, latent, cells = hidden_codes.shape
    hid, chan = w_in.shape[0], w_out.shape[0]
    nblk = pl.cdiv(cells, BLK)
    pad = nblk * BLK
    return pl.pallas_call(
        lambda *refs: fwd_kernel(cells, *refs),
        grid=(members, nblk),
        in_specs=[
            pl.BlockSpec((1, latent, BLK), lambda m, j: (m, 0, j)),
            pl.BlockSpec((hid, latent), lambda m, j: (0, 0)),
            pl.BlockSpec((hid, 128), lambda m, j: (0, 0)),
            pl.BlockSpec((chan, hid), lambda m, j: (0, 0)),
            pl.BlockSpec((chan, 1), lambda m, j: (0, 0)),
        ],
        out_specs=[
            pl.BlockSpec((2, 1, chan, BLK // 2), lambda m, j: (j, m, 0, 0)),
            pl.BlockSpec((1, hid, BLK), lambda m, j: (m, 0, j)),
            pl.BlockSpec((1, hid, BLK), lambda m, j: (m, 0, j)),
        ],
        out_shape=[
            jax.ShapeDtypeStruct((2 * nblk, members, chan, BLK // 2), BF16),
            jax.ShapeDtypeStruct((members, hid, pad), BF16),
            jax.ShapeDtypeStruct((members, hid, pad), BF16),
        ],
        compiler_params=pltpu.CompilerParams(dimension_semantics=("arbitrary", "arbitrary")),
        name="decoder_forward",
    )(hidden_codes, w_in, b_wide, w_out, b_out)


def slope(d):
    return d * lax.rsqrt(d * d + 0.0625)


def pair_kernel(cells, me_ref, area_ref, f_ref, t_ref, d_ref):
    groups, local, chan, wide = f_ref.shape
    members = groups * local
    me = me_ref[0]

    def strip(i, carry):
        rows = pl.ds(pl.multiple_of(i * 8, 8), 8)
        for l in range(wide // 128):
            lanes = pl.ds(l * 128, 128)
            v = [f_ref[m // local, m % local, rows, lanes].astype(F32) for m in range(members)]
            total = [None] * members
            for m in range(members):
                for q in range(m + 1, members):
                    s = slope(v[m] - v[q])
                    total[m] = s if total[m] is None else total[m] + s
                    total[q] = -s if total[q] is None else total[q] - s
            goal = t_ref[rows, lanes].astype(F32)
            cell = lax.broadcasted_iota(jnp.int32, (8, 128), 1) + (me * wide + l * 128)
            area = jnp.where(cell < LON, area_ref[0], area_ref[1])
            for m in range(members):
                d = area * (slope(v[m] - goal) - total[m] * (1.0 / members))
                d = jnp.where(cell < cells, d, 0.0)
                d_ref[m // local, m % local, rows, lanes] = d.astype(BF16)
        return carry

    lax.fori_loop(0, chan // 8, strip, 0)


def pair_gradient(me, area, block, target):
    groups, local, chan, wide = block.shape
    cells = target.shape[1]
    return pl.pallas_call(
        lambda *refs: pair_kernel(cells, *refs),
        grid_spec=pltpu.PrefetchScalarGridSpec(
            num_scalar_prefetch=2,
            grid=(1,),
            in_specs=[
                pl.BlockSpec(block.shape, lambda i, me, area: (0, 0, 0, 0)),
                pl.BlockSpec((chan, wide), lambda i, me, area: (0, me[0])),
            ],
            out_specs=pl.BlockSpec(block.shape, lambda i, me, area: (0, 0, 0, 0)),
        ),
        out_shape=jax.ShapeDtypeStruct(block.shape, BF16),
        name="pair_gradient",
    )(me, area, block, target)


def bwd_kernel(cells, d_ref, act_ref, gp_ref, hc_ref, w_out_t_ref, w_in_t_ref, cs_ref, g_ref, dpre_ref):
    hid = dpre_ref.shape[0]
    latent = hc_ref.shape[1]
    chan = d_ref.shape[2]
    nt = (((1,), (1,)), ((), ()))
    first = (pl.program_id(0) == 0) & (pl.program_id(1) == 0)

    @pl.when(first)
    def _():
        g_ref[...] = jnp.zeros_like(g_ref)

    hc = hc_ref[0]
    lane = lax.broadcasted_iota(jnp.int32, hc.shape, 1) + pl.program_id(1) * BLK
    hc = jnp.where(lane < cells, hc, jnp.zeros_like(hc))
    d = jnp.concatenate([d_ref[0, 0], d_ref[1, 0]], axis=1)
    d = jnp.concatenate([d, jnp.zeros((128 - chan, BLK), BF16)], axis=0)
    bias_lane = lax.broadcasted_iota(jnp.int32, (SUB, 128), 1) == chan
    for k in range(hid // SUB):
        rows = pl.ds(k * SUB, SUB)
        dact = jnp.dot(w_out_t_ref[rows, :], d, preferred_element_type=F32)
        dpre = dact * gp_ref[0, rows, :].astype(F32)
        dpre_b = dpre.astype(BF16)
        dpre_ref[rows, :] = dpre_b
        part = dpre[:, :128]
        for l in range(1, BLK // 128):
            part = part + dpre[:, l * 128 : (l + 1) * 128]
        bias = jnp.sum(part, axis=1, keepdims=True)
        g_ref[rows, :latent] += lax.dot_general(dpre_b, hc, nt, preferred_element_type=F32)
        out = lax.dot_general(act_ref[0, rows, :], d, nt, preferred_element_type=F32)
        g_ref[rows, latent:] += jnp.where(bias_lane, bias, out)
    cs = jnp.dot(w_in_t_ref[...], dpre_ref[...], preferred_element_type=F32)
    cs_ref[0] = cs.astype(BF16)


def decoder_backward(dfor, act, gp, hidden_codes, w_out_t, w_in_t):
    members, latent, cells = hidden_codes.shape
    hid = act.shape[1]
    chan = dfor.shape[2]
    nblk = pl.cdiv(cells, BLK)
    return pl.pallas_call(
        lambda *refs: bwd_kernel(cells, *refs),
        grid=(members, nblk),
        in_specs=[
            pl.BlockSpec((2, 1, chan, BLK // 2), lambda m, j: (j, m, 0, 0)),
            pl.BlockSpec((1, hid, BLK), lambda m, j: (m, 0, j)),
            pl.BlockSpec((1, hid, BLK), lambda m, j: (m, 0, j)),
            pl.BlockSpec((1, latent, BLK), lambda m, j: (m, 0, j)),
            pl.BlockSpec((hid, 128), lambda m, j: (0, 0)),
            pl.BlockSpec((latent, hid), lambda m, j: (0, 0)),
        ],
        out_specs=[
            pl.BlockSpec((1, latent, BLK), lambda m, j: (m, 0, j)),
            pl.BlockSpec((hid, latent + 128), lambda m, j: (0, 0)),
        ],
        out_shape=[
            jax.ShapeDtypeStruct((members, latent, cells), BF16),
            jax.ShapeDtypeStruct((hid, latent + 128), F32),
        ],
        scratch_shapes=[pltpu.VMEM((hid, BLK), BF16)],
        compiler_params=pltpu.CompilerParams(dimension_semantics=("arbitrary", "arbitrary")),
        name="decoder_backward",
    )(dfor, act, gp, hidden_codes, w_out_t, w_in_t)


def total_gradient(grads, scale):
    hid, wide = grads.shape
    half = hid // 2
    chips = lax.axis_size(CHIPS)
    core = lax.axis_index("c")
    swap = [(0, 1), (1, 0)]
    keep = lax.dynamic_slice(grads, (core * half, 0), (half, wide))
    give = lax.dynamic_slice(grads, ((1 - core) * half, 0), (half, wide)).astype(BF16)
    both = keep + lax.ppermute(give, "c", swap).astype(F32)
    shares = both.astype(BF16).reshape(chips, half // chips, wide)
    shares = lax.all_to_all(shares, CHIPS, 0, 0, tiled=True)
    share = (jnp.sum(shares.astype(F32), axis=0) * scale).astype(BF16)
    mine = lax.all_to_all(
        jnp.broadcast_to(share[None], (chips, *share.shape)), CHIPS, 0, 0, tiled=True
    ).reshape(half, wide)
    other = lax.ppermute(mine, "c", swap)
    low = jnp.where(core == 0, mine, other)
    high = jnp.where(core == 0, other, mine)
    return jnp.concatenate([low, high], axis=0).astype(F32)


def on_device(hidden_codes, w_in, b_in, w_out, b_out, target, band_start):
    local, latent, cells = hidden_codes.shape
    chan = w_out.shape[0]
    rows = cells // LON
    lat_rows = rows * lax.axis_size(SPACE)
    members = local * lax.axis_size(MEMBER)
    angle = ((band_start[0] + jnp.arange(rows, dtype=jnp.int32)).astype(F32) + 0.5) * (
        math.pi / lat_rows
    ) - math.pi / 2
    area = jnp.cos(angle)
    me = lax.axis_index(MEMBER).astype(jnp.int32).reshape(1)
    b_wide = jnp.broadcast_to(b_in[:, None], (b_in.shape[0], 128))
    w_out_t = jnp.pad(w_out.T, ((0, 0), (0, 128 - chan)))
    forecast, act, gp = decoder_forward(hidden_codes, w_in, b_wide, w_out, b_out[:, None])
    block = lax.all_to_all(forecast, MEMBER, 0, 0, tiled=True)
    dfor = pair_gradient(me, area, block, target)
    dfor = lax.all_to_all(dfor, MEMBER, 0, 0, tiled=True)
    code_sensitivity, grads = decoder_backward(dfor, act, gp, hidden_codes, w_out_t, w_in.T)
    total = total_gradient(grads, 1.0 / math.sqrt(members * cells))
    return (
        code_sensitivity,
        total[:, :latent],
        total[:, latent : latent + chan].T,
        total[:, latent + chan],
    )


def solution(mesh):
    fine = Mesh(mesh.devices.reshape([n for _, n in FINE]), [a for a, _ in FINE])
    in_specs = (P(MEMBER, None, SPACE), P(), P(), P(), P(), P(None, SPACE), P(SPACE))
    out_specs = (P(MEMBER, None, SPACE), P(), P(), P())
    return jax.shard_map(
        on_device, mesh=fine, in_specs=in_specs, out_specs=out_specs, check_vma=False
    )
```

```python
import math

import jax
import jax.numpy as jnp
from jax import lax
from jax.experimental import pallas as pl
from jax.experimental.pallas import tpu as pltpu
from jax.sharding import Mesh
from jax.sharding import PartitionSpec as P

LON = 1440
PER = 360
BLK = 2 * PER
BBLK = 4 * PER
SUB = 256
FSUB = 512
C0 = math.sqrt(2.0 / math.pi)
C1 = C0 * 0.044715
F32 = jnp.float32
BF16 = jnp.bfloat16
NT = (((1,), (1,)), ((), ()))

FINE = (("y", 4), ("xl", 2), ("z", 8), ("xh", 2), ("c", 2))
MEMBER = ("y", "xl")
SPACE = ("z", "xh", "c")
PLANE = ("y", "xl", "xh")


VMEM = pl.BlockSpec(memory_space=pltpu.VMEM)
SMEM = pl.BlockSpec(memory_space=pltpu.SMEM)


def on_chip(x):
    return pltpu.with_memory_space_constraint(x, pltpu.VMEM)


def limit(mib):
    return pltpu.CompilerParams(vmem_limit_bytes=mib * 2**20)


def whole(shape):
    return pl.BlockSpec(shape, lambda *a: (0,) * len(shape))


def halved(w):
    return (w.astype(F32) * 0.5).astype(BF16)


def column(row):
    return jnp.broadcast_to(row, (128, row.shape[1])).T


def fwd_kernel(hc_ref, w_in_ref, b_ref, w_out_ref, bo_ref, f_ref, wide_ref):
    hid = w_in_ref.shape[0]
    cells = hc_ref.shape[1]
    for i in range(hid // 128):
        rows = pl.ds(i * 128, 128)
        wide_ref[rows, :] = column(b_ref[:, rows])
    hc = hc_ref[0]
    half_out = halved(w_out_ref[...])
    f = None
    for k in range(hid // FSUB):
        rows = pl.ds(k * FSUB, FSUB)
        pre = lax.dot_general(w_in_ref[rows, :], hc, NT, preferred_element_type=F32)
        b = jnp.concatenate([wide_ref[rows, :]] * pl.cdiv(cells, 128), axis=1)[:, :cells]
        x = pre + b
        t = jnp.tanh(x * (C1 * (x * x) + C0))
        act = (x * (t + 1.0)).astype(BF16)
        part = jnp.dot(half_out[:, k * FSUB : (k + 1) * FSUB], act, preferred_element_type=F32)
        f = part if f is None else f + part
    f = (f + column(bo_ref[...])[:, :1]).astype(BF16)
    for i in range(cells // PER):
        f_ref[i, 0] = f[:, i * PER : (i + 1) * PER]


def decoder_forward(codes, w_in, b_in, w_out, b_out):
    members, cells, latent = codes.shape
    hid, chan = w_in.shape[0], w_out.shape[0]
    groups = cells // PER
    return pl.pallas_call(
        fwd_kernel,
        grid=(members,),
        in_specs=[
            pl.BlockSpec((1, cells, latent), lambda m: (m, 0, 0)),
            whole(w_in.shape),
            whole(b_in.shape),
            whole(w_out.shape),
            whole(b_out.shape),
        ],
        out_specs=pl.BlockSpec((groups, 1, chan, PER), lambda m: (0, m, 0, 0)),
        out_shape=jax.ShapeDtypeStruct((groups, members, chan, PER), BF16),
        scratch_shapes=[pltpu.VMEM((hid, 128), F32)],
        compiler_params=pltpu.CompilerParams(dimension_semantics=("arbitrary",)),
        name="decoder_forward",
    )(codes, w_in, b_in, w_out, b_out)


def gate_kernel(hc_ref, w_in_ref, b_ref, *refs):
    act_ref, gp_ref = refs[-2:]
    hid = w_in_ref.shape[0]
    hc = hc_ref[0]
    for k in range(hid // SUB):
        rows = pl.ds(k * SUB, SUB)
        pre = lax.dot_general(hc, w_in_ref[rows, :], NT, preferred_element_type=F32)
        x = pre + b_ref[:, rows]
        x2 = x * x
        t = jnp.tanh(x * (C1 * x2 + C0))
        p = t + 1.0
        a = x * p
        act_ref[0, :, rows] = a.astype(BF16)
        gp_ref[0, :, rows] = a * (1.0 - t) * ((3.0 * C1) * x2 + C0) + p


def decoder_gates(member, codes, w_in, b_in, so_far=()):
    members, cells, latent = codes.shape
    hid = w_in.shape[0]
    return pl.pallas_call(
        gate_kernel,
        grid=(cells // BLK,),
        in_specs=[
            pl.BlockSpec((1, BLK, latent), lambda j: (member, j, 0)),
            whole(w_in.shape),
            whole(b_in.shape),
        ]
        + [pl.BlockSpec(memory_space=pl.ANY)] * len(so_far),
        out_specs=[pl.BlockSpec((1, BLK, hid), lambda j: (member, j, 0))] * 2,
        out_shape=[
            jax.ShapeDtypeStruct((members, cells, hid), BF16),
            jax.ShapeDtypeStruct((members, cells, hid), F32),
        ],
        input_output_aliases={3 + i: i for i in range(len(so_far))},
        compiler_params=pltpu.CompilerParams(dimension_semantics=("arbitrary",)),
        cost_estimate=pl.CostEstimate(flops=8 * 10**9, transcendentals=3 * 10**6, bytes_accessed=20 * 10**6),
        name=f"decoder_gates_{member}",
    )(codes, w_in, b_in, *so_far)


def slope(d):
    return d * lax.rsqrt(d * d + 0.0625)


def pair_kernel(me_ref, area_ref, f_ref, t_ref, d_ref):
    groups, local, chan, wide = f_ref.shape
    members = groups * local
    me = me_ref[0]

    def strip(i, carry):
        rows = pl.ds(pl.multiple_of(i * 8, 8), 8)
        for l in range(0, wide, 128):
            n = min(128, wide - l)
            lanes = pl.ds(l, n)
            v = [f_ref[m // local, m % local, rows, lanes].astype(F32) for m in range(members)]
            total = [None] * members
            for m in range(members):
                for q in range(m + 1, members):
                    s = slope(v[m] - v[q])
                    total[m] = s if total[m] is None else total[m] + s
                    total[q] = -s if total[q] is None else total[q] - s
            goal = t_ref[rows, lanes].astype(F32)
            cell = lax.broadcasted_iota(jnp.int32, (8, n), 1) + (me * wide + l)
            area = jnp.where(cell < LON, area_ref[0], area_ref[1])
            for m in range(members):
                d = area * (slope(v[m] - goal) - total[m] * (1.0 / members))
                d_ref[m // local, m % local, rows, lanes] = d.astype(BF16)
        return carry

    lax.fori_loop(0, chan // 8, strip, 0)


def pair_gradient(me, area, block, goal):
    return pl.pallas_call(
        pair_kernel,
        in_specs=[SMEM, SMEM, VMEM, VMEM],
        out_specs=VMEM,
        out_shape=pltpu.VMEM(block.shape, BF16),
        compiler_params=limit(8),
        name="pair_gradient",
    )(me, area, on_chip(block), goal)


def bwd_kernel(d_ref, act_ref, gp_ref, hc_ref, w_out_ref, w_in_ref, cs_ref, g_ref, dpre_ref):
    hid, latent = w_in_ref.shape
    chan = w_out_ref.shape[0]
    first = (pl.program_id(0) == 0) & (pl.program_id(1) == 0)

    @pl.when(first)
    def _():
        g_ref[...] = jnp.zeros_like(g_ref)

    d = jnp.concatenate([d_ref[i, 0] for i in range(d_ref.shape[0])], axis=1)
    d_t = d.astype(F32).T.astype(BF16)
    hc_t = hc_ref[0].astype(F32).T.astype(BF16)
    left = jnp.concatenate([hc_t, jnp.ones((16, hc_t.shape[1]), BF16)], axis=0)
    half_out = halved(w_out_ref[...])
    bias_end = latent + 8

    def slab(k):
        cols = pl.ds(k * SUB, SUB)
        dact = jnp.dot(d_t, half_out[:, k * SUB : (k + 1) * SUB], preferred_element_type=F32)
        dpre_ref[:, cols] = (dact * gp_ref[0, :, cols]).astype(BF16)

    slab(0)
    for k in range(hid // SUB):
        if k + 1 < hid // SUB:
            slab(k + 1)
        cols = pl.ds(k * SUB, SUB)
        g_in = jnp.dot(left, dpre_ref[:, cols], preferred_element_type=F32)
        g_out = jnp.dot(d, act_ref[0, :, cols], preferred_element_type=F32)
        for i in range(SUB // 128):
            c = k * (SUB // 128) + i
            half, base = c // 4, (c % 4) * (bias_end + chan)
            lanes = slice(i * 128, (i + 1) * 128)
            g_ref[half, base : base + bias_end, :] += g_in[:bias_end, lanes]
            g_ref[half, base + bias_end : base + bias_end + chan, :] += g_out[:, lanes]
    cs = jnp.dot(dpre_ref[...], w_in_ref[...], preferred_element_type=F32)
    cs_ref[0] = cs.astype(BF16)


def decoder_backward(dfor, act, gp, codes, w_out, w_in):
    members, cells, latent = codes.shape
    hid = act.shape[2]
    chan = dfor.shape[2]
    rows = hid // 2 * (latent + 8 + chan) // 128
    return pl.pallas_call(
        bwd_kernel,
        grid=(members, cells // BBLK),
        in_specs=[
            pl.BlockSpec((BBLK // PER, 1, chan, PER), lambda m, j: (j, m, 0, 0)),
            pl.BlockSpec((1, BBLK, hid), lambda m, j: (m, j, 0)),
            pl.BlockSpec((1, BBLK, hid), lambda m, j: (m, j, 0)),
            pl.BlockSpec((1, BBLK, latent), lambda m, j: (m, j, 0)),
            whole(w_out.shape),
            whole(w_in.shape),
        ],
        out_specs=[
            pl.BlockSpec((1, BBLK, latent), lambda m, j: (m, j, 0)),
            whole((2, rows, 128)),
        ],
        out_shape=[
            jax.ShapeDtypeStruct((members, cells, latent), BF16),
            jax.ShapeDtypeStruct((2, rows, 128), F32),
        ],
        scratch_shapes=[pltpu.VMEM((BBLK, hid), BF16)],
        compiler_params=pltpu.CompilerParams(dimension_semantics=("arbitrary", "arbitrary")),
        name="decoder_backward",
    )(dfor, act, gp, codes, w_out, w_in)


def unpack_kernel(core_ref, mine_ref, other_ref, gi_ref, go_ref, gb_ref):
    chan = go_ref.shape[0]
    latent = gi_ref.shape[1]
    per = latent + 8 + chan
    lower = core_ref[0] == 0
    for c in range(8):
        rows = pl.ds((c % 4) * per, per)
        a, b = mine_ref[rows, :].astype(F32), other_ref[rows, :].astype(F32)
        x = jnp.where(lower == (c < 4), a, b)
        cols = slice(c * 128, (c + 1) * 128)
        gi_ref[cols, :] = x[:latent].T
        gb_ref[:, cols] = x[latent : latent + 1]
        go_ref[:, cols] = x[latent + 8 :] * 0.5


def unpack(core, mine, other, hid, latent, chan):
    return pl.pallas_call(
        unpack_kernel,
        in_specs=[SMEM, VMEM, VMEM],
        out_specs=[VMEM] * 3,
        out_shape=[
            jax.ShapeDtypeStruct((hid, latent), F32),
            jax.ShapeDtypeStruct((chan, hid), F32),
            jax.ShapeDtypeStruct((1, hid), F32),
        ],
        name="unpack_gradients",
    )(core, on_chip(mine), on_chip(other))


def total_gradient(grads, scale):
    _, rows, lanes = grads.shape
    plane = lax.axis_size(PLANE)
    per = -(-rows // (8 * plane)) * 8
    core = lax.axis_index("c")
    swap = [(0, 1), (1, 0)]
    keep = lax.dynamic_index_in_dim(grads, core, 0, keepdims=False)
    give = lax.dynamic_index_in_dim(grads, 1 - core, 0, keepdims=False).astype(BF16)
    both = (keep + lax.ppermute(give, "c", swap).astype(F32)).astype(BF16)
    both = jnp.pad(both, ((0, plane * per - rows), (0, 0))).reshape(plane, per, lanes)
    shares = lax.all_to_all(both, PLANE, 0, 0, tiled=True)
    share = jnp.sum(shares.astype(F32), axis=0)
    parts = lax.all_to_all(
        jnp.broadcast_to(share[None], (lax.axis_size("z"), *share.shape)), "z", 0, 0, tiled=True
    )
    share = (jnp.sum(parts, axis=0) * scale).astype(BF16)
    mine = lax.all_to_all(
        jnp.broadcast_to(share[None], (plane, *share.shape)), PLANE, 0, 0, tiled=True
    ).reshape(plane * per, lanes)[:rows]
    return mine, lax.ppermute(mine, "c", swap)


def on_device(hidden_codes, w_in, b_in, w_out, b_out, target, band_start):
    local, latent, cells = hidden_codes.shape
    hid, chan = w_in.shape[0], w_out.shape[0]
    rows = cells // LON
    lat_rows = rows * lax.axis_size(SPACE)
    members = local * lax.axis_size(MEMBER)
    angle = ((band_start[0] + jnp.arange(rows, dtype=jnp.int32)).astype(F32) + 0.5) * (
        math.pi / lat_rows
    ) - math.pi / 2
    area = jnp.cos(angle)
    me = lax.axis_index(MEMBER).astype(jnp.int32)
    codes = jnp.swapaxes(hidden_codes, 1, 2)
    b_row = b_in[None, :]
    forecast = decoder_forward(codes, w_in, b_row, w_out, b_out[None, :])
    block = lax.all_to_all(forecast, MEMBER, 0, 0, tiled=True)
    gates = decoder_gates(0, codes, w_in, b_row)
    goal = lax.dynamic_slice(target, (0, me * PER), (chan, PER))
    block, gates = lax.optimization_barrier((block, gates))
    dfor = pair_gradient(me.reshape(1), area, block, goal)
    dfor_in = lax.all_to_all(dfor, MEMBER, 0, 0, tiled=True)
    later_b, _ = lax.optimization_barrier((b_row, dfor))
    act, gp = decoder_gates(1, codes, w_in, later_b, gates)
    sensitivity, grads = decoder_backward(dfor_in, act, gp, codes, w_out, w_in)
    mine, other = total_gradient(grads, 1.0 / math.sqrt(members * cells))
    core = lax.axis_index("c").astype(jnp.int32).reshape(1)
    grad_in, grad_out, grad_b = unpack(core, mine, other, hid, latent, chan)
    return jnp.swapaxes(sensitivity, 1, 2), grad_in, grad_out, grad_b[0]


def solution(mesh):
    fine = Mesh(mesh.devices.reshape([n for _, n in FINE]), [a for a, _ in FINE])
    in_specs = (P(MEMBER, None, SPACE), P(), P(), P(), P(), P(None, SPACE), P(SPACE))
    out_specs = (P(MEMBER, None, SPACE), P(), P(), P())
    return jax.shard_map(
        on_device, mesh=fine, in_specs=in_specs, out_specs=out_specs, check_vma=False
    )
```

```python
import math

import jax
import jax.numpy as jnp
from jax import lax
from jax.experimental import pallas as pl
from jax.experimental.pallas import tpu as pltpu
from jax.sharding import Mesh
from jax.sharding import PartitionSpec as P

LON = 1440
PER = 360
BLK = 2 * PER
BBLK = 4 * PER
SUB = 256
FSUB = 512
C0 = math.sqrt(2.0 / math.pi)
C1 = C0 * 0.044715
F32 = jnp.float32
BF16 = jnp.bfloat16
NT = (((1,), (1,)), ((), ()))

FINE = (("y", 4), ("xl", 2), ("z", 8), ("xh", 2), ("c", 2))
MEMBER = ("y", "xl")
SPACE = ("z", "xh", "c")
PLANE = ("y", "xl", "xh")


VMEM = pl.BlockSpec(memory_space=pltpu.VMEM)
SMEM = pl.BlockSpec(memory_space=pltpu.SMEM)


def on_chip(x):
    return pltpu.with_memory_space_constraint(x, pltpu.VMEM)


def limit(mib):
    return pltpu.CompilerParams(vmem_limit_bytes=mib * 2**20)


def whole(shape):
    return pl.BlockSpec(shape, lambda *a: (0,) * len(shape))


def halved(w):
    return (w.astype(F32) * 0.5).astype(BF16)


def column(row):
    return jnp.broadcast_to(row, (128, row.shape[1])).T


def fwd_kernel(hc_ref, w_in_ref, b_ref, w_out_ref, bo_ref, f_ref, wide_ref):
    hid = w_in_ref.shape[0]
    cells = hc_ref.shape[1]
    for i in range(hid // 128):
        rows = pl.ds(i * 128, 128)
        wide_ref[rows, :] = column(b_ref[:, rows])
    hc = hc_ref[0]
    half_out = halved(w_out_ref[...])
    f = None
    for k in range(hid // FSUB):
        rows = pl.ds(k * FSUB, FSUB)
        pre = lax.dot_general(w_in_ref[rows, :], hc, NT, preferred_element_type=F32)
        b = jnp.concatenate([wide_ref[rows, :]] * pl.cdiv(cells, 128), axis=1)[:, :cells]
        x = pre + b
        t = jnp.tanh(x * (C1 * (x * x) + C0))
        act = (x * (t + 1.0)).astype(BF16)
        part = jnp.dot(half_out[:, k * FSUB : (k + 1) * FSUB], act, preferred_element_type=F32)
        f = part if f is None else f + part
    f = (f + column(bo_ref[...])[:, :1]).astype(BF16)
    for i in range(cells // PER):
        f_ref[i, 0] = f[:, i * PER : (i + 1) * PER]


def decoder_forward(codes, w_in, b_in, w_out, b_out):
    members, cells, latent = codes.shape
    hid, chan = w_in.shape[0], w_out.shape[0]
    groups = cells // PER
    return pl.pallas_call(
        fwd_kernel,
        grid=(members,),
        in_specs=[
            pl.BlockSpec((1, cells, latent), lambda m: (m, 0, 0)),
            whole(w_in.shape),
            whole(b_in.shape),
            whole(w_out.shape),
            whole(b_out.shape),
        ],
        out_specs=pl.BlockSpec((groups, 1, chan, PER), lambda m: (0, m, 0, 0)),
        out_shape=jax.ShapeDtypeStruct((groups, members, chan, PER), BF16),
        scratch_shapes=[pltpu.VMEM((hid, 128), F32)],
        compiler_params=pltpu.CompilerParams(dimension_semantics=("arbitrary",)),
        name="decoder_forward",
    )(codes, w_in, b_in, w_out, b_out)


def gate_kernel(hc_ref, w_in_ref, b_ref, *refs):
    act_ref, gp_ref = refs[-2:]
    hid = w_in_ref.shape[0]
    hc = hc_ref[0]
    for k in range(hid // SUB):
        rows = pl.ds(k * SUB, SUB)
        pre = lax.dot_general(hc, w_in_ref[rows, :], NT, preferred_element_type=F32)
        x = pre + b_ref[:, rows]
        x2 = x * x
        t = jnp.tanh(x * (C1 * x2 + C0))
        p = t + 1.0
        a = x * p
        act_ref[0, :, rows] = a.astype(BF16)
        gp_ref[0, :, rows] = a * (1.0 - t) * ((3.0 * C1) * x2 + C0) + p


def decoder_gates(member, codes, w_in, b_in, so_far=()):
    members, cells, latent = codes.shape
    hid = w_in.shape[0]
    return pl.pallas_call(
        gate_kernel,
        grid=(cells // BLK,),
        in_specs=[
            pl.BlockSpec((1, BLK, latent), lambda j: (member, j, 0)),
            whole(w_in.shape),
            whole(b_in.shape),
        ]
        + [pl.BlockSpec(memory_space=pl.ANY)] * len(so_far),
        out_specs=[pl.BlockSpec((1, BLK, hid), lambda j: (member, j, 0))] * 2,
        out_shape=[
            jax.ShapeDtypeStruct((members, cells, hid), BF16),
            jax.ShapeDtypeStruct((members, cells, hid), F32),
        ],
        input_output_aliases={3 + i: i for i in range(len(so_far))},
        compiler_params=pltpu.CompilerParams(dimension_semantics=("arbitrary",)),
        cost_estimate=pl.CostEstimate(flops=8 * 10**9, transcendentals=3 * 10**6, bytes_accessed=20 * 10**6),
        name=f"decoder_gates_{member}",
    )(codes, w_in, b_in, *so_far)


def slope(d):
    return d * lax.rsqrt(d * d + 0.0625)


def pair_kernel(me_ref, area_ref, f_ref, t_ref, d_ref):
    groups, local, chan, wide = f_ref.shape
    members = groups * local
    me = me_ref[0]

    def strip(i, carry):
        rows = pl.ds(pl.multiple_of(i * 8, 8), 8)
        for l in range(0, wide, 128):
            n = min(128, wide - l)
            lanes = pl.ds(l, n)
            v = [f_ref[m // local, m % local, rows, lanes].astype(F32) for m in range(members)]
            total = [None] * members
            for m in range(members):
                for q in range(m + 1, members):
                    s = slope(v[m] - v[q])
                    total[m] = s if total[m] is None else total[m] + s
                    total[q] = -s if total[q] is None else total[q] - s
            goal = t_ref[rows, lanes].astype(F32)
            cell = lax.broadcasted_iota(jnp.int32, (8, n), 1) + (me * wide + l)
            area = jnp.where(cell < LON, area_ref[0], area_ref[1])
            for m in range(members):
                d = area * (slope(v[m] - goal) - total[m] * (1.0 / members))
                d_ref[m // local, m % local, rows, lanes] = d.astype(BF16)
        return carry

    lax.fori_loop(0, chan // 8, strip, 0)


def pair_gradient(me, area, block, goal):
    return pl.pallas_call(
        pair_kernel,
        in_specs=[SMEM, SMEM, VMEM, VMEM],
        out_specs=VMEM,
        out_shape=pltpu.VMEM(block.shape, BF16),
        compiler_params=limit(8),
        name="pair_gradient",
    )(me, area, on_chip(block), goal)


def bwd_kernel(core_ref, d_ref, act_ref, gp_ref, hc_ref, w_out_ref, w_in_ref, cs_ref, keep_ref, give_ref, g_ref, dpre_ref):
    hid, latent = w_in_ref.shape
    chan = w_out_ref.shape[0]
    per = hc_ref.shape[1] // PER
    m, j = pl.program_id(0), pl.program_id(1)
    first = (m == 0) & (j == 0)
    last = (m == pl.num_programs(0) - 1) & (j == pl.num_programs(1) - 1)

    @pl.when(first)
    def _():
        g_ref[...] = jnp.zeros_like(g_ref)

    d = jnp.concatenate([d_ref[j * per + i, m] for i in range(per)], axis=1)
    d_t = d.astype(F32).T.astype(BF16)
    hc_t = hc_ref[0].astype(F32).T.astype(BF16)
    left = jnp.concatenate([hc_t, jnp.ones((16, hc_t.shape[1]), BF16)], axis=0)
    half_out = halved(w_out_ref[...])
    bias_end = latent + 8

    def slab(k):
        cols = pl.ds(k * SUB, SUB)
        dact = jnp.dot(d_t, half_out[:, k * SUB : (k + 1) * SUB], preferred_element_type=F32)
        dpre_ref[:, cols] = (dact * gp_ref[0, :, cols]).astype(BF16)

    slab(0)
    for k in range(hid // SUB):
        if k + 1 < hid // SUB:
            slab(k + 1)
        cols = pl.ds(k * SUB, SUB)
        g_in = jnp.dot(left, dpre_ref[:, cols], preferred_element_type=F32)
        g_out = jnp.dot(d, act_ref[0, :, cols], preferred_element_type=F32)
        for i in range(SUB // 128):
            c = k * (SUB // 128) + i
            half, base = c // 4, (c % 4) * (bias_end + chan)
            lanes = slice(i * 128, (i + 1) * 128)
            g_ref[half, base : base + bias_end, :] += g_in[:bias_end, lanes]
            g_ref[half, base + bias_end : base + bias_end + chan, :] += g_out[:, lanes]
    cs = jnp.dot(dpre_ref[...], w_in_ref[...], preferred_element_type=F32)
    cs_ref[0] = cs.astype(BF16)

    @pl.when(last)
    def _():
        core = core_ref[0]
        keep_ref[...] = g_ref[core]
        give_ref[...] = g_ref[1 - core].astype(BF16)


def decoder_backward(core, dfor, act, gp, codes, w_out, w_in):
    members, cells, latent = codes.shape
    hid = act.shape[2]
    chan = dfor.shape[2]
    rows = hid // 2 * (latent + 8 + chan) // 128
    rows = -(-rows // (8 * lax.axis_size(PLANE))) * 8 * lax.axis_size(PLANE)
    return pl.pallas_call(
        bwd_kernel,
        grid=(members, cells // BBLK),
        in_specs=[
            SMEM,
            VMEM,
            pl.BlockSpec((1, BBLK, hid), lambda m, j: (m, j, 0)),
            pl.BlockSpec((1, BBLK, hid), lambda m, j: (m, j, 0)),
            pl.BlockSpec((1, BBLK, latent), lambda m, j: (m, j, 0)),
            whole(w_out.shape),
            whole(w_in.shape),
        ],
        out_specs=[
            pl.BlockSpec((1, BBLK, latent), lambda m, j: (m, j, 0)),
            VMEM,
            VMEM,
        ],
        out_shape=[
            jax.ShapeDtypeStruct((members, cells, latent), BF16),
            pltpu.VMEM((rows, 128), F32),
            pltpu.VMEM((rows, 128), BF16),
        ],
        scratch_shapes=[pltpu.VMEM((2, rows, 128), F32), pltpu.VMEM((BBLK, hid), BF16)],
        compiler_params=pltpu.CompilerParams(
            dimension_semantics=("arbitrary", "arbitrary"), vmem_limit_bytes=48 * 2**20
        ),
        name="decoder_backward",
    )(core, on_chip(dfor), act, gp, codes, *(pltpu.with_memory_space_constraint(w, pltpu.HBM) for w in (w_out, w_in)))


def unpack_kernel(core_ref, mine_ref, other_ref, gi_ref, go_ref, gb_ref):
    chan = go_ref.shape[0]
    latent = gi_ref.shape[1]
    per = latent + 8 + chan
    lower = core_ref[0] == 0
    for c in range(8):
        rows = pl.ds((c % 4) * per, per)
        a, b = mine_ref[rows, :].astype(F32), other_ref[rows, :].astype(F32)
        x = jnp.where(lower == (c < 4), a, b)
        cols = slice(c * 128, (c + 1) * 128)
        gi_ref[cols, :] = x[:latent].T
        gb_ref[:, cols] = x[latent : latent + 1]
        go_ref[:, cols] = x[latent + 8 :] * 0.5


def unpack(core, mine, other, hid, latent, chan):
    return pl.pallas_call(
        unpack_kernel,
        in_specs=[SMEM, VMEM, VMEM],
        out_specs=[VMEM] * 3,
        out_shape=[
            jax.ShapeDtypeStruct((hid, latent), F32),
            jax.ShapeDtypeStruct((chan, hid), F32),
            jax.ShapeDtypeStruct((1, hid), F32),
        ],
        compiler_params=limit(8),
        name="unpack_gradients",
    )(core, on_chip(mine), on_chip(other))


def total_gradient(keep, give, scale):
    rows, lanes = keep.shape
    plane = lax.axis_size(PLANE)
    swap = [(0, 1), (1, 0)]
    both = (keep + lax.ppermute(give, "c", swap).astype(F32)).astype(BF16)
    shares = lax.all_to_all(both.reshape(plane, rows // plane, lanes), PLANE, 0, 0, tiled=True)
    share = (jnp.sum(shares.astype(F32), axis=0) * 0.5).astype(BF16)
    parts = lax.all_to_all(
        jnp.broadcast_to(share[None], (lax.axis_size("z"), *share.shape)), "z", 0, 0, tiled=True
    )
    share = (jnp.sum(parts.astype(F32), axis=0) * (2.0 * scale)).astype(BF16)
    mine = lax.all_to_all(
        jnp.broadcast_to(share[None], (plane, *share.shape)), PLANE, 0, 0, tiled=True
    ).reshape(rows, lanes)
    return mine, lax.ppermute(mine, "c", swap)


def on_device(hidden_codes, w_in, b_in, w_out, b_out, target, band_start):
    local, latent, cells = hidden_codes.shape
    hid, chan = w_in.shape[0], w_out.shape[0]
    rows = cells // LON
    lat_rows = rows * lax.axis_size(SPACE)
    members = local * lax.axis_size(MEMBER)
    angle = ((band_start[0] + jnp.arange(rows, dtype=jnp.int32)).astype(F32) + 0.5) * (
        math.pi / lat_rows
    ) - math.pi / 2
    area = jnp.cos(angle)
    me = lax.axis_index(MEMBER).astype(jnp.int32)
    codes = jnp.swapaxes(hidden_codes, 1, 2)
    b_row = b_in[None, :]
    forecast = decoder_forward(codes, w_in, b_row, w_out, b_out[None, :])
    block = lax.all_to_all(forecast, MEMBER, 0, 0, tiled=True)
    gates = decoder_gates(0, codes, w_in, b_row)
    goal = lax.dynamic_slice(target, (0, me * PER), (chan, PER))
    block, gates = lax.optimization_barrier((block, gates))
    dfor = pair_gradient(me.reshape(1), area, block, goal)
    dfor_in = lax.all_to_all(dfor, MEMBER, 0, 0, tiled=True)
    later_b, _ = lax.optimization_barrier((b_row, dfor))
    act, gp = decoder_gates(1, codes, w_in, later_b, gates)
    core = lax.axis_index("c").astype(jnp.int32).reshape(1)
    sensitivity, keep, give = decoder_backward(core, dfor_in, act, gp, codes, w_out, w_in)
    mine, other = total_gradient(keep, give, 1.0 / math.sqrt(members * cells))
    grad_in, grad_out, grad_b = unpack(core, mine, other, hid, latent, chan)
    return jnp.swapaxes(sensitivity, 1, 2), grad_in, grad_out, grad_b[0]


def solution(mesh):
    fine = Mesh(mesh.devices.reshape([n for _, n in FINE]), [a for a, _ in FINE])
    in_specs = (P(MEMBER, None, SPACE), P(), P(), P(), P(), P(None, SPACE), P(SPACE))
    out_specs = (P(MEMBER, None, SPACE), P(), P(), P())
    return jax.shard_map(
        on_device, mesh=fine, in_specs=in_specs, out_specs=out_specs, check_vma=False
    )
```

```python
import math

import jax
import jax.numpy as jnp
from jax import lax
from jax.experimental import pallas as pl
from jax.experimental.pallas import tpu as pltpu
from jax.sharding import Mesh
from jax.sharding import PartitionSpec as P

LON = 1440
PER = 360
BLK = 2 * PER
BBLK = 4 * PER
SUB = 256
BSUB = 512
FSUB = 1024
C0 = math.sqrt(2.0 / math.pi)
C1 = C0 * 0.044715
F32 = jnp.float32
BF16 = jnp.bfloat16
NT = (((1,), (1,)), ((), ()))

FINE = (("y", 4), ("xl", 2), ("z", 8), ("xh", 2), ("c", 2))
MEMBER = ("y", "xl")
SPACE = ("z", "xh", "c")
PLANE = ("y", "xl", "xh")


VMEM = pl.BlockSpec(memory_space=pltpu.VMEM)
SMEM = pl.BlockSpec(memory_space=pltpu.SMEM)


def on_chip(x):
    return pltpu.with_memory_space_constraint(x, pltpu.VMEM)


def limit(mib):
    return pltpu.CompilerParams(vmem_limit_bytes=mib * 2**20)


def whole(shape):
    return pl.BlockSpec(shape, lambda *a: (0,) * len(shape))


def halved(w):
    return (w.astype(F32) * 0.5).astype(BF16)


def column(row):
    return jnp.broadcast_to(row, (128, row.shape[1])).T


def fwd_kernel(hc_ref, w_in_ref, b_ref, w_out_ref, bo_ref, f_ref, wide_ref):
    hid = w_in_ref.shape[0]
    cells = hc_ref.shape[1]
    for i in range(hid // 128):
        rows = pl.ds(i * 128, 128)
        wide_ref[rows, :] = column(b_ref[:, rows])
    hc = hc_ref[0]
    half_out = halved(w_out_ref[...])
    f = None
    for k in range(hid // FSUB):
        rows = pl.ds(k * FSUB, FSUB)
        pre = lax.dot_general(w_in_ref[rows, :], hc, NT, preferred_element_type=F32)
        b = jnp.concatenate([wide_ref[rows, :]] * pl.cdiv(cells, 128), axis=1)[:, :cells]
        x = pre + b
        t = jnp.tanh(x * (C1 * (x * x) + C0))
        act = (x * (t + 1.0)).astype(BF16)
        part = jnp.dot(half_out[:, k * FSUB : (k + 1) * FSUB], act, preferred_element_type=F32)
        f = part if f is None else f + part
    f = (f + column(bo_ref[...])[:, :1]).astype(BF16)
    for i in range(cells // PER):
        f_ref[i, 0] = f[:, i * PER : (i + 1) * PER]


def decoder_forward(codes, w_in, b_in, w_out, b_out):
    members, cells, latent = codes.shape
    hid, chan = w_in.shape[0], w_out.shape[0]
    groups = cells // PER
    return pl.pallas_call(
        fwd_kernel,
        grid=(members,),
        in_specs=[
            pl.BlockSpec((1, cells, latent), lambda m: (m, 0, 0)),
            whole(w_in.shape),
            whole(b_in.shape),
            whole(w_out.shape),
            whole(b_out.shape),
        ],
        out_specs=pl.BlockSpec((groups, 1, chan, PER), lambda m: (0, m, 0, 0)),
        out_shape=jax.ShapeDtypeStruct((groups, members, chan, PER), BF16),
        scratch_shapes=[pltpu.VMEM((hid, 128), F32)],
        compiler_params=pltpu.CompilerParams(dimension_semantics=("arbitrary",)),
        name="decoder_forward",
    )(codes, w_in, b_in, w_out, b_out)


def gate_kernel(hc_ref, w_in_ref, b_ref, *refs):
    act_ref, gp_ref = refs[-2:]
    hid = w_in_ref.shape[0]
    hc = hc_ref[0]
    for k in range(hid // SUB):
        rows = pl.ds(k * SUB, SUB)
        pre = lax.dot_general(hc, w_in_ref[rows, :], NT, preferred_element_type=F32)
        x = pre + b_ref[:, rows]
        x2 = x * x
        t = jnp.tanh(x * (C1 * x2 + C0))
        p = t + 1.0
        a = x * p
        act_ref[0, :, rows] = a.astype(BF16)
        gp_ref[0, :, rows] = a * (1.0 - t) * ((3.0 * C1) * x2 + C0) + p


def decoder_gates(member, codes, w_in, b_in, so_far=()):
    members, cells, latent = codes.shape
    hid = w_in.shape[0]
    return pl.pallas_call(
        gate_kernel,
        grid=(cells // BLK,),
        in_specs=[
            pl.BlockSpec((1, BLK, latent), lambda j: (member, j, 0)),
            whole(w_in.shape),
            whole(b_in.shape),
        ]
        + [pl.BlockSpec(memory_space=pl.ANY)] * len(so_far),
        out_specs=[pl.BlockSpec((1, BLK, hid), lambda j: (member, j, 0))] * 2,
        out_shape=[
            jax.ShapeDtypeStruct((members, cells, hid), BF16),
            jax.ShapeDtypeStruct((members, cells, hid), F32),
        ],
        input_output_aliases={3 + i: i for i in range(len(so_far))},
        compiler_params=pltpu.CompilerParams(dimension_semantics=("arbitrary",)),
        cost_estimate=pl.CostEstimate(flops=8 * 10**9, transcendentals=3 * 10**6, bytes_accessed=20 * 10**6),
        name=f"decoder_gates_{member}",
    )(codes, w_in, b_in, *so_far)


def slope(d):
    return d * lax.rsqrt(d * d + 0.0625)


def pair_kernel(me_ref, area_ref, f_ref, t_ref, d_ref):
    groups, local, chan, wide = f_ref.shape
    members = groups * local
    me = me_ref[0]

    def strip(i, carry):
        rows = pl.ds(pl.multiple_of(i * 8, 8), 8)
        for l in range(0, wide, 128):
            n = min(128, wide - l)
            lanes = pl.ds(l, n)
            v = [f_ref[m // local, m % local, rows, lanes].astype(F32) for m in range(members)]
            total = [None] * members
            for m in range(members):
                for q in range(m + 1, members):
                    s = slope(v[m] - v[q])
                    total[m] = s if total[m] is None else total[m] + s
                    total[q] = -s if total[q] is None else total[q] - s
            goal = t_ref[rows, lanes].astype(F32)
            cell = lax.broadcasted_iota(jnp.int32, (8, n), 1) + (me * wide + l)
            area = jnp.where(cell < LON, area_ref[0], area_ref[1])
            for m in range(members):
                d = area * (slope(v[m] - goal) - total[m] * (1.0 / members))
                d_ref[m // local, m % local, rows, lanes] = d.astype(BF16)
        return carry

    lax.fori_loop(0, chan // 8, strip, 0, unroll=3)


def pair_gradient(me, area, block, goal):
    return pl.pallas_call(
        pair_kernel,
        in_specs=[SMEM, SMEM, VMEM, VMEM],
        out_specs=VMEM,
        out_shape=pltpu.VMEM(block.shape, BF16),
        compiler_params=limit(8),
        name="pair_gradient",
    )(me, area, on_chip(block), goal)


def bwd_kernel(core_ref, d_ref, act_ref, gp_ref, hc_ref, w_out_ref, w_in_ref, cs_ref, keep_ref, give_ref, g_ref, dpre_ref):
    hid, latent = w_in_ref.shape
    chan = w_out_ref.shape[0]
    per = hc_ref.shape[1] // PER
    m, j = pl.program_id(0), pl.program_id(1)
    first = (m == 0) & (j == 0)
    last = (m == pl.num_programs(0) - 1) & (j == pl.num_programs(1) - 1)

    @pl.when(first)
    def _():
        g_ref[...] = jnp.zeros_like(g_ref)

    d = jnp.concatenate([d_ref[j * per + i, m] for i in range(per)], axis=1)
    d_t = d.astype(F32).T.astype(BF16)
    hc_t = hc_ref[0].astype(F32).T.astype(BF16)
    left = jnp.concatenate([hc_t, jnp.ones((16, hc_t.shape[1]), BF16)], axis=0)
    half_out = halved(w_out_ref[...])
    bias_end = latent + 8

    def slab(k):
        cols = pl.ds(k * BSUB, BSUB)
        dact = jnp.dot(d_t, half_out[:, k * BSUB : (k + 1) * BSUB], preferred_element_type=F32)
        dpre_ref[:, cols] = (dact * gp_ref[0, :, cols]).astype(BF16)

    slab(0)
    for k in range(hid // BSUB):
        if k + 1 < hid // BSUB:
            slab(k + 1)
        cols = pl.ds(k * BSUB, BSUB)
        g_in = jnp.dot(left, dpre_ref[:, cols], preferred_element_type=F32)
        g_out = jnp.dot(d, act_ref[0, :, cols], preferred_element_type=F32)
        for i in range(BSUB // 128):
            c = k * (BSUB // 128) + i
            half, base = c // 4, (c % 4) * (bias_end + chan)
            lanes = slice(i * 128, (i + 1) * 128)
            g_ref[half, base : base + bias_end, :] += g_in[:bias_end, lanes]
            g_ref[half, base + bias_end : base + bias_end + chan, :] += g_out[:, lanes]
    cs = jnp.dot(dpre_ref[...], w_in_ref[...], preferred_element_type=F32)
    cs_ref[0] = cs.astype(BF16)

    @pl.when(last)
    def _():
        core = core_ref[0]
        keep_ref[...] = g_ref[core]
        give_ref[...] = g_ref[1 - core].astype(BF16)


def decoder_backward(core, dfor, act, gp, codes, w_out, w_in):
    members, cells, latent = codes.shape
    hid = act.shape[2]
    chan = dfor.shape[2]
    rows = hid // 2 * (latent + 8 + chan) // 128
    rows = -(-rows // (8 * lax.axis_size(PLANE))) * 8 * lax.axis_size(PLANE)
    return pl.pallas_call(
        bwd_kernel,
        grid=(members, cells // BBLK),
        in_specs=[
            SMEM,
            VMEM,
            pl.BlockSpec((1, BBLK, hid), lambda m, j: (m, j, 0)),
            pl.BlockSpec((1, BBLK, hid), lambda m, j: (m, j, 0)),
            pl.BlockSpec((1, BBLK, latent), lambda m, j: (m, j, 0)),
            whole(w_out.shape),
            whole(w_in.shape),
        ],
        out_specs=[
            pl.BlockSpec((1, BBLK, latent), lambda m, j: (m, j, 0)),
            VMEM,
            VMEM,
        ],
        out_shape=[
            jax.ShapeDtypeStruct((members, cells, latent), BF16),
            pltpu.VMEM((rows, 128), F32),
            pltpu.VMEM((rows, 128), BF16),
        ],
        scratch_shapes=[pltpu.VMEM((2, rows, 128), F32), pltpu.VMEM((BBLK, hid), BF16)],
        compiler_params=pltpu.CompilerParams(
            dimension_semantics=("arbitrary", "arbitrary"), vmem_limit_bytes=48 * 2**20
        ),
        name="decoder_backward",
    )(core, on_chip(dfor), act, gp, codes, *(pltpu.with_memory_space_constraint(w, pltpu.HBM) for w in (w_out, w_in)))


def unpack_kernel(core_ref, mine_ref, other_ref, gi_ref, go_ref, gb_ref):
    chan = go_ref.shape[0]
    latent = gi_ref.shape[1]
    per = latent + 8 + chan
    lower = core_ref[0] == 0
    for c in range(8):
        rows = pl.ds((c % 4) * per, per)
        a, b = mine_ref[rows, :].astype(F32), other_ref[rows, :].astype(F32)
        x = jnp.where(lower == (c < 4), a, b)
        cols = slice(c * 128, (c + 1) * 128)
        gi_ref[cols, :] = x[:latent].T
        gb_ref[:, cols] = x[latent : latent + 1]
        go_ref[:, cols] = x[latent + 8 :] * 0.5


def unpack(core, mine, other, hid, latent, chan):
    return pl.pallas_call(
        unpack_kernel,
        in_specs=[SMEM, VMEM, VMEM],
        out_specs=[VMEM] * 3,
        out_shape=[
            jax.ShapeDtypeStruct((hid, latent), F32),
            jax.ShapeDtypeStruct((chan, hid), F32),
            jax.ShapeDtypeStruct((1, hid), F32),
        ],
        compiler_params=limit(8),
        name="unpack_gradients",
    )(core, on_chip(mine), on_chip(other))


def total_gradient(keep, give, scale):
    rows, lanes = keep.shape
    plane = lax.axis_size(PLANE)
    swap = [(0, 1), (1, 0)]
    both = (keep + lax.ppermute(give, "c", swap).astype(F32)).astype(BF16)
    shares = lax.all_to_all(both.reshape(plane, rows // plane, lanes), PLANE, 0, 0, tiled=True)
    share = (jnp.sum(shares.astype(F32), axis=0) * 0.5).astype(BF16)
    parts = lax.all_to_all(
        jnp.broadcast_to(share[None], (lax.axis_size("z"), *share.shape)), "z", 0, 0, tiled=True
    )
    share = (jnp.sum(parts.astype(F32), axis=0) * (2.0 * scale)).astype(BF16)
    mine = lax.all_to_all(
        jnp.broadcast_to(share[None], (plane, *share.shape)), PLANE, 0, 0, tiled=True
    ).reshape(rows, lanes)
    return mine, lax.ppermute(mine, "c", swap)


def on_device(hidden_codes, w_in, b_in, w_out, b_out, target, band_start):
    local, latent, cells = hidden_codes.shape
    hid, chan = w_in.shape[0], w_out.shape[0]
    rows = cells // LON
    lat_rows = rows * lax.axis_size(SPACE)
    members = local * lax.axis_size(MEMBER)
    angle = ((band_start[0] + jnp.arange(rows, dtype=jnp.int32)).astype(F32) + 0.5) * (
        math.pi / lat_rows
    ) - math.pi / 2
    area = jnp.cos(angle)
    me = lax.axis_index(MEMBER).astype(jnp.int32)
    codes = jnp.swapaxes(hidden_codes, 1, 2)
    b_row = b_in[None, :]
    forecast = decoder_forward(codes, w_in, b_row, w_out, b_out[None, :])
    block = lax.all_to_all(forecast, MEMBER, 0, 0, tiled=True)
    gates = decoder_gates(0, codes, w_in, b_row)
    goal = lax.dynamic_slice(target, (0, me * PER), (chan, PER))
    block, gates = lax.optimization_barrier((block, gates))
    dfor = pair_gradient(me.reshape(1), area, block, goal)
    dfor_in = lax.all_to_all(dfor, MEMBER, 0, 0, tiled=True)
    later_b, _ = lax.optimization_barrier((b_row, dfor))
    act, gp = decoder_gates(1, codes, w_in, later_b, gates)
    core = lax.axis_index("c").astype(jnp.int32).reshape(1)
    sensitivity, keep, give = decoder_backward(core, dfor_in, act, gp, codes, w_out, w_in)
    mine, other = total_gradient(keep, give, 1.0 / math.sqrt(members * cells))
    grad_in, grad_out, grad_b = unpack(core, mine, other, hid, latent, chan)
    return jnp.swapaxes(sensitivity, 1, 2), grad_in, grad_out, grad_b[0]


def solution(mesh):
    fine = Mesh(mesh.devices.reshape([n for _, n in FINE]), [a for a, _ in FINE])
    in_specs = (P(MEMBER, None, SPACE), P(), P(), P(), P(), P(None, SPACE), P(SPACE))
    out_specs = (P(MEMBER, None, SPACE), P(), P(), P())
    return jax.shard_map(
        on_device, mesh=fine, in_specs=in_specs, out_specs=out_specs, check_vma=False
    )
```
